32 devices in a mesh: row: 4 (over z), col: 4 (over x, core), depth: 2 (over y).
Axes of the slice: x: 2, y: 2, z: 4, core: 2. Of those that a mesh axis runs over, the one named last changes fastest.
Arguments:
- tokens: bfloat16 [2048, 8192], P(('row', 'col'), 'depth'), may hold values from -0.3125 to 0.3125
- weight: bfloat16 [8192, 8192], P('depth', ('col', 'row')), may hold values from -0.0625 to 0.0625
- grad_output: bfloat16 [2048, 8192], P('row', ('col', 'depth')), may hold values from -6 to 6
Outputs:
- grad_input: bfloat16 [2048, 8192], P(('row', 'col'), 'depth')
- grad_weight: bfloat16 [8192, 8192], P('depth', ('col', 'row'))
The draws below stay inside these ranges and needn't reach their ends.
All inputs are finite; a program needn't handle non-finite values.
Results may differ from the reference program's by a relative error of at most 0.001.
Values may be sent and summed in bfloat16 or wider, within the bound.
A program may use at most 128 MiB of HBM per device.

```python
import jax
import jax.numpy as jnp

D_IN = 8192
D_OUT = 8192
TOKENS = 2048


def spiked(drawn, stream_key, source, target, parts, factor):
    def block_of(axis_at):
        return (jnp.arange(drawn.shape[axis_at]) // (drawn.shape[axis_at] // parts)).reshape((-1,) + (1,) * (drawn.ndim - 1 - axis_at))

    one_side = jax.random.permutation(stream_key, parts)[block_of(target)]
    other_side = (block_of(target) + parts // 2) % parts
    return jnp.where((block_of(source) == one_side) | (block_of(source) == other_side), factor * drawn, drawn)


def shard_levels(rng, extent, pieces, low, top_value):
    gain, own = 1.0, jax.random.fold_in(rng, 6)
    for position, shards_of in pieces:
        steps = jnp.exp(jax.random.uniform(jax.random.fold_in(own, position), (shards_of,), jnp.float32, low / len(pieces), top_value / len(pieces)))
        gain = gain * jnp.repeat(steps, extent[position] // shards_of).reshape([-1 if axis == position else 1 for axis in range(len(extent))])
    return gain


def bell_draw(rng, dims, width, reach, pieces=(), kind=jnp.bfloat16):
    factor_of = shard_levels(rng, dims, pieces, -0.22, 0.18) if pieces else 1.0
    result = jax.random.normal(rng, dims, jnp.float32) * width * factor_of
    return jnp.minimum(jnp.maximum(result, -reach), reach).astype(kind)


def bell_draw_with(stream_key, shape, width, most, pieces, heavy, held_as=jnp.bfloat16):
    drawn = width * jax.random.normal(stream_key, shape, jnp.float32)
    if pieces:
        drawn = drawn * shard_levels(stream_key, shape, pieces, -0.22, 0.18)
    return jnp.clip(spiked(drawn, jax.random.fold_in(stream_key, 3), *heavy), -most, most).astype(held_as)


def setup_inputs(seed: int = 0) -> dict:
    keys = jax.random.split(jax.random.key(seed), 4)
    tokens = bell_draw(keys[0], (TOKENS, D_IN), (TOKENS ** -0.5), 0.3125, ((0, 16), (1, 2)))
    weight = bell_draw(keys[1], (D_IN, D_OUT), D_IN ** -0.5, 0.0625, ((0, 2), (1, 16)))
    grad_output = bell_draw_with(keys[2], (TOKENS, D_OUT), 1.0, 6.0, ((0, 4), (1, 8)), (1, 0, 8, 2.0))
    return {"tokens": tokens, "weight": weight, "grad_output": grad_output}


def reference(tokens, weight, grad_output):
    grad_input = jnp.dot(grad_output, weight.T, preferred_element_type=jnp.float32).astype(jnp.bfloat16)
    grad_weight = jnp.dot(tokens.T, grad_output, preferred_element_type=jnp.float32).astype(jnp.bfloat16)
    return grad_input, grad_weight
```

```python
import jax
import jax.numpy as jnp
from jax import lax
from jax.sharding import PartitionSpec as P


last_with_last = (((1,), (1,)), ((), ()))
first_with_first = (((0,), (0,)), ((), ()))
CHUNKS = 4


def input_grads(weight, grad_block):
    weight_block = lax.all_gather(weight, "row", axis=1, tiled=True)
    partial_value = lax.dot_general(
        grad_block, weight_block, last_with_last, preferred_element_type=jnp.float32
    )
    column_slab = lax.psum_scatter(partial_value, "col", scatter_dimension=1, tiled=True).astype(
        jnp.bfloat16
    )
    return lax.all_to_all(column_slab, "col", split_axis=0, concat_axis=1, tiled=True)


def weight_grads(tokens, grad_block):
    partial_value = lax.dot_general(
        lax.all_gather(tokens, "col", axis=0, tiled=True),
        grad_block,
        first_with_first,
        preferred_element_type=jnp.float32,
    )
    return lax.psum_scatter(partial_value, "row", scatter_dimension=1, tiled=True).astype(
        jnp.bfloat16
    )


def per_device_general(tokens, weight, grad_output):
    grad_block = lax.all_gather(grad_output, "depth", axis=1, tiled=True)
    grad_input = input_grads(weight, grad_block)
    grad_weight = weight_grads(tokens, grad_block)
    return (grad_input, grad_weight)


def along_row(value, step):
    return lax.ppermute(value, "row", [(i, (i + step) % 4) for i in range(4)])


def next_row(value, sign, reach):
    pairs = [(i, i + 1) for i in range(4 - reach)]
    return lax.ppermute(value, "row", pairs if sign > 0 else [(3 - i, 3 - j) for i, j in pairs])


def across_col(value, bits):
    return lax.ppermute(value, "col", [(i, i ^ bits) for i in range(4)])


def gather_row(block, row):
    up, down = [block], [block]
    for step in (1, 2, 3):
        sources = range(step - 1, 3)
        up.append(lax.ppermute(up[-1], "row", [(i, i + 1) for i in sources]))
        down.append(lax.ppermute(down[-1], "row", [(3 - i, 2 - i) for i in sources]))
    return [block] + [jnp.where(row >= s, up[s], down[4 - s]) for s in (1, 2, 3)]


def scatter_row(terms):
    up = next_row(terms[1], 1, 3)
    down = next_row(terms[3], -1, 3)
    up = next_row(terms[2] + up, 1, 2)
    down = next_row(terms[2] + down, -1, 2)
    up = next_row(terms[3] + up, 1, 1)
    down = next_row(terms[1] + down, -1, 1)
    return terms[0] + up + down


def per_device_fours(tokens, weight, grad_output):
    return fours(tokens, weight, grad_output)


def fours(tokens, weight, grad_output):
    row, col, depth = lax.axis_index("row"), lax.axis_index("col"), lax.axis_index("depth")
    rows, width = tokens.shape[0], weight.shape[1]

    size = weight.shape[0] // CHUNKS
    chunks = []
    for j in range(CHUNKS):
        w0 = weight[j * size : (j + 1) * size]
        w2 = across_col(w0, 2)
        chunks.append([w0, across_col(w0, 1), w2, across_col(w2, 1)])

    other = lax.ppermute(grad_output, "depth", [(0, 1), (1, 0)])
    first = depth == 0
    grad_block = jnp.concatenate(
        [jnp.where(first, grad_output, other), jnp.where(first, other, grad_output)], axis=1
    )

    def columns_of(step):
        at = lax.rem(row + step, 4) * width
        return lax.dynamic_slice_in_dim(grad_block, at, width, axis=1)

    mine = [columns_of(0)]
    for s in (1, 2, 3):
        mine.append(along_row(columns_of(s), s))

    def of_col(bits):
        at = jnp.bitwise_xor(col, bits) * rows
        return [lax.dynamic_slice_in_dim(g, at, rows, axis=0) for g in mine]

    by_col = [of_col(bits) for bits in range(4)]

    packed = [jnp.concatenate(blocks) for blocks in by_col]
    held = [packed[0]]
    for bits in (1, 2, 3):
        held.append(across_col(packed[bits], bits))
    columns = []
    for chunk in chunks:
        total = sum(
            lax.dot_general(g, w, last_with_last, preferred_element_type=jnp.float32)
            for g, w in zip(held, chunk)
        )
        terms = [total[s * rows : (s + 1) * rows] for s in range(4)]
        columns.append(scatter_row(terms).astype(jnp.bfloat16))
    grad_input = jnp.concatenate(columns, axis=1)

    blocks = gather_row(tokens, row)
    near, far = [], []
    for block in blocks:
        near.append(across_col(block, 1))
        block_x = across_col(block, 2)
        far.append((block_x, across_col(block_x, 1)))
    groups = (
        (blocks + near, by_col[0] + by_col[1]),
        ([v for pair in far[:2] for v in pair], [by_col[b][s] for s in (0, 1) for b in (2, 3)]),
        ([v for pair in far[2:] for v in pair], [by_col[b][s] for s in (2, 3) for b in (2, 3)]),
    )
    total = None
    for a, g in groups:
        value = lax.dot_general(
            jnp.concatenate(a),
            jnp.concatenate(g),
            first_with_first,
            preferred_element_type=jnp.float32,
        )
        total = value if total is None else total + value
    return grad_input, total.astype(jnp.bfloat16)


def solution(mesh):
    fours_fit = mesh.shape["row"] == 4 and mesh.shape["col"] == 4 and mesh.shape["depth"] == 2
    return jax.shard_map(
        per_device_fours if fours_fit else per_device_general,
        mesh=mesh,
        in_specs=(
            P(("row", "col"), "depth"),
            P("depth", ("col", "row")),
            P("row", ("col", "depth")),
        ),
        out_specs=(P(("row", "col"), "depth"), P("depth", ("col", "row"))),
        check_vma=False,
    )
```
